512 devices in a mesh: xy: 64 (over y, z_lo, core), gz: 8 (over x, z_hi).
Axes of the slice: x: 4, y: 8, z: 8 (z_hi: 2, z_lo: 4; z = z_hi * 4 + z_lo), core: 2. Of those that a mesh axis runs over, the one named last changes fastest.
Arguments:
- positions: float32 [3, 32, 8, 64, 128], P(None, None, 'gz', 'xy'), may hold values from 0 to 2
- velocities: float32 [3, 32, 8, 64, 128], P(None, None, 'gz', 'xy'), may hold values from -6 to 6
- forces_prev: float32 [3, 32, 8, 64, 128], P(None, None, 'gz', 'xy'), may hold values from -48 to 48
- seeds: int32 [32, 8, 64, 128], P(None, 'gz', 'xy'), may hold values from 0 to 16383
- counts: int32 [8, 64, 128], P('gz', 'xy'), may hold values from 12 to 32, as said below
- offsets: int32 [2], replicated, may hold values from 0 to 127
Outputs:
- forces: float32 [3, 32, 8, 64, 128], P(None, None, 'gz', 'xy')
- velocities_out: float32 [3, 32, 8, 64, 128], P(None, None, 'gz', 'xy')
- stress: float32 [6, 8, 64, 128], P(None, 'gz', 'xy')
The draws below stay inside these ranges and needn't reach their ends.
Inputs may be any that keep to these rules, and one draw needn't show every extreme that they name: `counts`: each cell holds 12 to 32 beads; every row of 128 cells along x has a full cell.
All inputs are finite; a program needn't handle non-finite values.
Results may differ from the reference program's by a relative error of at most 0.0003.
Values sent between devices are 32-bit elements; how exact they have to be, the bound alone decides.
A program may use at most 128 MiB of HBM per device.

```python
import math
import jax
import jax.numpy as jnp
from jax import lax

SLOTS = 32
NX = 128
NY = 64
NZ = 8


def draw_counts(key, part):
    first_key = jax.random.fold_in(key, 11)
    second_key = jax.random.fold_in(key, 23)
    base = jax.random.randint(first_key, (NZ, NY, NX), 3 * SLOTS // 8, SLOTS + 1, dtype=jnp.int32)
    spot = jax.random.randint(second_key, (NZ, NY, 1), 0, NX, dtype=jnp.int32)
    full = jnp.arange(NX, dtype=jnp.int32)[None, None, :] == spot
    return jnp.where(full, SLOTS, base).astype(jnp.int32)


def place_ends(drawn, own_key, smallest, top_value):
    shape = drawn.shape
    place = [jax.random.randint(jax.random.fold_in(own_key, axis), (), 0, shape[axis]) for axis in range(len(shape))]
    drawn = drawn.at[tuple(place)].set(smallest)
    longest = shape.index(max(shape))
    place[longest] = (place[longest] + 1) % shape[longest]
    return drawn.at[tuple(place)].set(top_value)


def block_levels(key, dims, split, least, top_value):
    level, own = 1.0, jax.random.fold_in(key, 6)
    for axis_at, blocks in split:
        steps = jnp.exp(jax.random.uniform(jax.random.fold_in(own, axis_at), (blocks,), jnp.float32, least / len(split), top_value / len(split)))
        level = level * jnp.repeat(steps, dims[axis_at] // blocks).reshape([-1 if axis == axis_at else 1 for axis in range(len(dims))])
    return level


def normal_values(key, dims, scale, limit, split=(), held_as=jnp.bfloat16):
    values = jax.random.normal(key, dims, jnp.float32) * scale
    if len(split) > 0:
        values = block_levels(key, dims, split, -0.22, 0.18) * values
    return jnp.clip(values, min=-limit, max=limit).astype(held_as)


def setup_inputs(seed: int = 0) -> dict:
    arg_keys = jax.random.split(jax.random.key(seed), 7)
    return {
        "positions": jnp.clip(2.0 * jax.random.uniform(arg_keys[0], (3, SLOTS, NZ, NY, NX), jnp.float32) ** block_levels(arg_keys[0], (3, SLOTS, NZ, NY, NX), ((2, 8), (3, 64)), -0.2, 0.2), 0.0, 2.0),
        "velocities": normal_values(arg_keys[1], (3, SLOTS, NZ, NY, NX), 1.0, 6.0, ((2, 8), (3, 64)), jnp.float32),
        "forces_prev": normal_values(arg_keys[2], (3, SLOTS, NZ, NY, NX), 8.0, 48.0, ((2, 8), (3, 64)), jnp.float32),
        "seeds": place_ends(jax.random.randint(arg_keys[3], (SLOTS, NZ, NY, NX), 0, 16384), jax.random.fold_in(arg_keys[3], 1), 0, 16383).astype(jnp.int32),
        "counts": draw_counts(jax.random.fold_in(arg_keys[6], 71), 0),
        "offsets": jax.random.randint(arg_keys[5], (2,), 0, NX).astype(jnp.int32),
    }


CONSERVATIVE = 25.0
FRICTION = 4.5
NOISE_LEVEL = 3.0
TIME_STEP = 0.04
SHEAR_SPEED = 1.0
CELL_VOLUME = 8.0
FLOOR_SQUARED = 0.0025
COMPONENT_PAIRS = [(0, 0), (1, 1), (2, 2), (0, 1), (0, 2), (1, 2)]
NEIGHBOURS = [(dz, dy, dx) for dz in (-1, 0, 1) for dy in (-1, 0, 1) for dx in (-1, 0, 1)]

def pair_terms(home_beads, near_beads, offset, same_cell, step):
    slots = home_beads.shape[1]
    shift = jnp.asarray([offset[0], offset[1], offset[2]], jnp.float32)[:, None, None, None]
    separation = home_beads[0:3, :, None, :] - near_beads[0:3, None, :, :] - 2.0 * shift
    velocity_gap = home_beads[3:6, :, None, :] - near_beads[3:6, None, :, :]
    squared = lax.optimization_barrier(jnp.sum(separation * separation, axis=0))
    distance = jnp.sqrt(jnp.maximum(squared, FLOOR_SQUARED))
    occupied = home_beads[7][:, None, :] * near_beads[7][None, :, :]
    if same_cell:
        occupied = occupied * (1.0 - jnp.eye(slots, dtype=jnp.float32))[:, :, None]
    weight = jnp.maximum(1.0 - distance, 0.0) * occupied
    seed_sum = home_beads[6].astype(jnp.int32)[:, None, :] + near_beads[6].astype(jnp.int32)[None, :, :] + (7919 * step + 1)
    hashed = seed_sum * (seed_sum + 1) % 65521
    noise = (hashed.astype(jnp.float32) / 65521.0 - 0.5) * math.sqrt(12.0)
    approach = lax.optimization_barrier(jnp.sum(separation * velocity_gap, axis=0)) / distance
    magnitude = (CONSERVATIVE * weight - FRICTION * weight * weight * approach + NOISE_LEVEL * weight * noise / math.sqrt(TIME_STEP)) / distance
    pair_force = magnitude[None] * separation
    home_force = lax.optimization_barrier(jnp.sum(pair_force, axis=2))
    near_force = -lax.optimization_barrier(jnp.sum(pair_force, axis=1))
    virial = jnp.stack([lax.optimization_barrier(jnp.sum(separation[first] * pair_force[second], axis=(0, 1))) for first, second in COMPONENT_PAIRS]) * (0.5 / CELL_VOLUME)
    return (home_force, near_force, virial)

def build_ghosts(state, offset_now):
    shear = jnp.asarray([0.0, 0.0, 0.0, SHEAR_SPEED, 0.0, 0.0, 0.0, 0.0], jnp.float32)[:, None, None, None, None]
    lower = jnp.roll(state[:, :, :, -1:, :], -offset_now, axis=-1) - shear
    upper = jnp.roll(state[:, :, :, :1, :], offset_now, axis=-1) + shear
    return jnp.concatenate([lower, state, upper], axis=3)

def evaluate(state, offset_now, step):
    extended = build_ghosts(state, offset_now)
    slots = state.shape[1]
    depth = state.shape[2]
    rows = state.shape[3]
    width = state.shape[4]

    def plane(level):
        home = lax.dynamic_index_in_dim(state, level, 2, keepdims=False).reshape(8, slots, -1)
        total_force = jnp.zeros((3, slots, rows * width), jnp.float32)
        total_virial = jnp.zeros((6, rows * width), jnp.float32)
        for dz, dy, dx in NEIGHBOURS:
            near_plane = lax.dynamic_index_in_dim(extended, (level + dz) % depth, 2, keepdims=False)
            near = jnp.roll(near_plane[:, :, 1 + dy:1 + dy + rows, :], -dx, axis=-1).reshape(8, slots, -1)
            same = (dz, dy, dx) == (0, 0, 0)
            home_force, near_force, virial = pair_terms(home, near, (dx, dy, dz), same, step)
            total_force = total_force + home_force
            total_virial = total_virial + virial
        return (total_force.reshape(3, slots, rows, width), total_virial.reshape(6, rows, width))
    planes_force, planes_virial = lax.map(plane, jnp.arange(depth, dtype=jnp.int32))
    return (jnp.moveaxis(planes_force, 0, 2), jnp.moveaxis(planes_virial, 0, 1))

def reference(positions, velocities, forces_prev, seeds, counts, offsets):
    present = (lax.broadcasted_iota(jnp.int32, seeds.shape, 0) < counts[None]).astype(jnp.float32)
    fixed_part = jnp.stack([seeds.astype(jnp.float32), present])
    position_now = positions
    velocity_now = velocities
    force_now = forces_prev
    stress = None
    for step in range(2):
        half_speed = velocity_now + 0.5 * TIME_STEP * force_now
        position_now = position_now + TIME_STEP * half_speed
        state = jnp.concatenate([position_now, half_speed, fixed_part], axis=0)
        force_now, stress = evaluate(state, offsets[step], step)
        velocity_now = half_speed + 0.5 * TIME_STEP * force_now
    return (force_now, velocity_now * present[None], stress)
```

```python
import functools
import math

import jax
import jax.numpy as jnp
from jax import lax
from jax.experimental import pallas as pl
from jax.experimental.pallas import tpu as pltpu
from jax.sharding import PartitionSpec as P

DT = 0.04
PRIME = 65521
FAR = 1048576.0
NOISE = 3.0 * math.sqrt(12.0) / math.sqrt(DT)
UNIT = NOISE / 2.0**32
BIAS = 32768
OFFSET = 25.0 / UNIT - BIAS
DRAG = 4.5 / UNIT
PAIRS = [(0, 0), (1, 1), (2, 2), (0, 1), (0, 2), (1, 2)]
LANES = 128
C = 4


def phase(x):
    rest = jnp.floor(x.astype(jnp.float32) * (225.0 / PRIME) + 0.5).astype(jnp.int32)
    return x * jnp.int32(65551) + rest


def roll(x, shift):
    return pltpu.roll(x, shift, axis=x.ndim - 1)


def kernel(
    ny, nz, pos, vel, frc, seeds, counts, offsets, f_out, v_out, s_out,
    snd0, snd1, yp0, yp1, ym0, ym1, zp0, zp1, ry0, ry1, rz0, rz1, vz,
    rfm0, rfm1, rfp0, rfp1, rzm0, rzm1, vzm,
    ig, ii, jof, joi, jzf, jzi, gpart, facc, jacc_o, jacc_z, vi, vj_o, vj_z, send, recv,
):
    iy = lax.axis_index("xy")
    iz = lax.axis_index("gz")
    up_y = {"xy": lax.rem(iy + 1, ny), "gz": iz}
    dn_y = {"xy": lax.rem(iy + ny - 1, ny), "gz": iz}
    up_z = {"xy": iy, "gz": lax.rem(iz + 1, nz)}
    dn_z = {"xy": iy, "gz": lax.rem(iz + nz - 1, nz)}
    barrier = pltpu.get_barrier_semaphore()
    for where in (up_y, dn_y, up_z, dn_z):
        pl.semaphore_signal(barrier, inc=1, device_id=where, device_id_type=pl.DeviceIdType.MESH)

    started = []

    def remote(src, dst, step, slot, where):
        copy = pltpu.make_async_remote_copy(
            src_ref=src, dst_ref=dst, send_sem=send.at[step, slot], recv_sem=recv.at[step, slot],
            device_id=where, device_id_type=pl.DeviceIdType.MESH,
        )
        started.append(copy)
        return copy

    slot_no = (
        lax.broadcasted_iota(jnp.int32, (C, 8, LANES), 0) * 8 + lax.broadcasted_iota(jnp.int32, (C, 8, LANES), 1)
    )
    present = slot_no < counts[...]

    def tile(g, jf, ji, dxi, c, react, at):
        force = [[jnp.zeros((8, LANES), jnp.float32) for _ in range(4)] for _ in range(3)]
        for j in range(8):
            near = [jnp.broadcast_to(jf[dxi, c, k, j : j + 1, :], (8, LANES)) for k in range(6)]
            seed_j = jnp.broadcast_to(ji[dxi, c, 0, j : j + 1, :], (8, LANES))
            base_j = jnp.broadcast_to(ji[dxi, c, 1, j : j + 1, :], (8, LANES))
            back = [None, None, None]
            for a in range(4):
                d = [ig[g, k, a] - near[k] for k in range(3)]
                u = [ig[g, 3 + k, a] - near[3 + k] for k in range(3)]
                square = d[0] * d[0] + d[1] * d[1] + d[2] * d[2]
                inverse = lax.rsqrt(jnp.maximum(square, 0.0025))
                gap = jnp.maximum(inverse - 1.0, 0.0)
                drag = d[0] * u[0] + d[1] * u[1] + d[2] * u[2]
                angle = ii[g, 0, a] * seed_j + (ii[g, 1, a] + base_j)
                size = gap * ((angle.astype(jnp.float32) + OFFSET) - gap * drag)
                for k in range(3):
                    part = size * d[k]
                    force[k][a] = force[k][a] + part
                    if react:
                        back[k] = part if back[k] is None else back[k] + part
            if react:
                for k in range(3):
                    gpart[at, k, 8 * j : 8 * j + 8, :] = back[k]
        total = None
        if react:
            total = []
            for k in range(3):
                rows = [gpart[at, k, pl.ds(s, 8, stride=8), :] for s in range(8)]
                while len(rows) > 1:
                    rows = [rows[i] + rows[i + 1] for i in range(0, len(rows), 2)]
                total.append(rows[0])
        return force, total

    def pair_virial(g, jf, dxi, c, force, total):
        out = []
        for first, second in PAIRS:
            part = None
            for a in range(4):
                term = ig[g, first, a] * force[second][a]
                part = term if part is None else part + term
            if total is None:
                part = part + part
            else:
                part = part - jf[dxi, c, first] * total[second]
            out.append(part)
        return out

    def add_force(g, forces):
        for k in range(3):
            for a in range(4):
                value = facc[g, k, a]
                for force in forces:
                    value = value + force[k][a]
                facc[g, k, a] = value

    def add_rows(ref, at, values):
        for k, value in enumerate(values):
            ref[(*at, k)] = ref[(*at, k)] + value

    def i_prep(g, block, seed, shift_y, shear, step, turn):
        for k in range(3):
            value = turn(block(k))
            if k == 1 and shift_y != 0.0:
                value = value + shift_y
            for a in range(4):
                ig[g, k, a] = value[a]
            speed = turn(block(3 + k))
            if k == 0 and shear is not None:
                speed = speed + shear
            speed = speed * DRAG
            for a in range(4):
                ig[g, 3 + k, a] = speed[a]
        first = turn(seed).astype(jnp.int32) + (7919 * step + 1)
        many = phase(2 * first + 1)
        alone = phase(first * (first + 1)) + jnp.int32(BIAS - 2**31)
        for a in range(4):
            ii[g, 0, a] = many[a]
            ii[g, 1, a] = alone[a]

    def j_prep(jf, c, value_of, shift_z):
        for k in range(6):
            value = value_of(c, k)
            if k == 2 and shift_z != 0.0:
                value = value + shift_z
            if k >= 3:
                value = value * DRAG
            for dxi in range(3):
                dx = dxi - 1
                moved = value if dx == 0 else roll(value, (-dx) % LANES)
                if k == 0 and dx != 0:
                    moved = moved + 2.0 * dx
                jf[dxi, c, k] = moved

    def j_seed(ji, c, seed):
        number = seed.astype(jnp.int32)
        base = phase(number * number)
        for dxi in range(3):
            dx = dxi - 1
            ji[dxi, c, 0] = number if dx == 0 else roll(number, (-dx) % LANES)
            ji[dxi, c, 1] = base if dx == 0 else roll(base, (-dx) % LANES)

    def back_to_place(values, dxi):
        dx = dxi - 1
        return [v if dx == 0 else roll(v, dx % LANES) for v in values]

    for step in range(2):
        last = step == 1
        snd, yp, ym, zp = (snd1, yp1, ym1, zp1) if last else (snd0, yp0, ym0, zp0)
        ry, rz, rfm, rfp, rzm = (ry1, rz1, rfm1, rfp1, rzm1) if last else (ry0, rz0, rfm0, rfp0, rzm0)
        for k in range(3):
            if not last:
                half = vel[k] + 0.5 * DT * frc[k]
                place = jnp.where(present, pos[k] + DT * half, FAR)
            else:
                half = v_out[k] + DT * f_out[k]
                old = jnp.stack([snd0[c, k] for c in range(C)])
                place = jnp.where(present, old + DT * half, FAR)
            for c in range(C):
                snd[c, k] = place[c]
                snd[c, 3 + k] = half[c]
        if not last:
            number = seeds[...].astype(jnp.float32)
            for c in range(C):
                snd[c, 6] = number[c]

        def own(k):
            return jnp.stack([snd[c, k] for c in range(C)])

        seed_own = jnp.stack([snd0[c, 6] for c in range(C)])
        i_prep(0, own, seed_own, 0.0, None, step, lambda v: v)
        if not last:
            pl.semaphore_wait(barrier, 4)
        send_z = [remote(snd.at[c], zp.at[c], step, c, dn_z) for c in range(C)]
        send_up = remote(snd, ym, step, 4, up_y)
        send_dn = remote(snd, yp, step, 5, dn_y)
        send_z[0].start()
        send_dn.start()
        send_up.start()
        for c in range(1, C):
            send_z[c].start()

        for c in range(C):
            j_prep(jof, c, lambda c, k: snd[c, k], 0.0)
            if not last:
                j_seed(joi, c, snd0[c, 6])
        zero = jnp.zeros((8, LANES), jnp.float32)
        for g in range(3):
            for k in range(3):
                for a in range(4):
                    facc[g, k, a] = zero
            if last:
                for k in range(6):
                    vi[g, k] = zero
                    vj_o[g, k] = zero
                    vj_z[g, k] = zero

        def own_body(c, carry):
            force, _ = tile(0, jof, joi, 1, c, False, 0)
            force_x, total_x = tile(0, jof, joi, 2, c, True, 0)
            add_force(0, [force, force_x])
            for k in range(3):
                jacc_o[0, c, k] = jnp.zeros((8, LANES), jnp.float32)
                jacc_o[1, c, k] = jnp.zeros((8, LANES), jnp.float32)
                jacc_o[2, c, k] = total_x[k]
            if last:
                add_rows(vi, (0,), pair_virial(0, jof, 1, c, force, None))
                part = pair_virial(0, jof, 2, c, force_x, total_x)
                add_rows(vi, (0,), part)
                add_rows(vj_o, (2,), part)
            return carry

        lax.fori_loop(0, C, own_body, 0)

        offset = offsets[step]
        turn_p = jnp.where(iy == ny - 1, offset, 0)
        turn_m = jnp.where(iy == 0, lax.rem(LANES - offset, LANES), 0)
        shear_p = jnp.where(iy == ny - 1, 1.0, 0.0)
        shear_m = jnp.where(iy == 0, -1.0, 0.0)

        def turned(amount):
            return lambda v: jnp.stack([roll(v[a], amount) for a in range(C)])

        send_dn.wait_recv()
        i_prep(
            1, lambda k: jnp.stack([yp[c, k] for c in range(C)]), jnp.stack([yp0[c, 6] for c in range(C)]),
            2.0, shear_p, step, turned(turn_p),
        )

        def multi(g, jf, ji, c, jacc, jat, vj):
            forces = []
            for dxi in range(3):
                force, total = tile(g, jf, ji, dxi, c, True, dxi)
                forces.append(force)
                add_rows(jacc, jat(dxi), total)
                if last:
                    part = pair_virial(g, jf, dxi, c, force, total)
                    add_rows(vi, (g,), part)
                    add_rows(vj, (dxi,), part)
            add_force(g, forces)

        def up_body(c, carry):
            multi(1, jof, joi, c, jacc_o, lambda dxi: (dxi, c), vj_o)
            return carry

        lax.fori_loop(0, C, up_body, 0)

        send_up.wait_recv()
        i_prep(
            2, lambda k: jnp.stack([ym[c, k] for c in range(C)]), jnp.stack([ym0[c, 6] for c in range(C)]),
            -2.0, shear_m, step, turned(turn_m),
        )

        give_z = [remote(rz.at[c], rzm.at[c], step, 6 + c, up_z) for c in range(C)]
        for c in range(C):
            send_z[c].wait_recv()
            j_prep(jzf, c, lambda c, k: zp[c, k], 2.0)
            if not last:
                j_seed(jzi, c, zp0[c, 6])
            for dxi in range(3):
                for k in range(3):
                    jacc_z[dxi, k] = zero

            def z_body(g, carry):
                multi(g, jzf, jzi, c, jacc_z, lambda dxi: (dxi,), vj_z)
                return carry

            lax.fori_loop(0, 3, z_body, 0)
            for k in range(3):
                value = zero
                for dxi in range(3):
                    value = value + back_to_place([jacc_z[dxi, k]], dxi)[0]
                rz[c, k] = value * (-UNIT)
            give_z[c].start()

        scale = UNIT * 0.5 / 8.0

        def virial_rows(ref, at):
            rows = [jnp.sum(ref[at, k], axis=0, keepdims=True) for k in range(6)]
            return jnp.concatenate(rows + [jnp.zeros((2, LANES), jnp.float32)], axis=0) * scale

        undo_p = lax.rem(LANES - turn_p, LANES)
        undo_m = lax.rem(LANES - turn_m, LANES)
        for n, (g, undo) in enumerate(((1, undo_p), (2, undo_m))):
            for k in range(3):
                for a in range(4):
                    ry[n, 4 * k + a] = roll(facc[g, k, a] * UNIT, undo)
            if last:
                ry[n, 12] = roll(virial_rows(vi, g), undo)
        give_up = remote(ry.at[0], rfm, step, 10, up_y)
        give_dn = remote(ry.at[1], rfp, step, 11, dn_y)
        give_up.start()
        give_dn.start()
        if last:
            value = zero
            for dxi in range(3):
                value = value + back_to_place([virial_rows(vj_z, dxi)], dxi)[0]
            vz[...] = value
            give_v = remote(vz, vzm, step, 12, up_z)
            give_v.start()

        mine = [[facc[0, k, a] for a in range(4)] for k in range(3)]
        for dxi in range(3):
            for k in range(3):
                moved = back_to_place([jacc_o[dxi, a, k] for a in range(4)], dxi)
                mine[k] = [mine[k][a] - moved[a] for a in range(4)]
        if last:
            stress = virial_rows(vi, 0)
            for dxi in range(3):
                stress = stress + back_to_place([virial_rows(vj_o, dxi)], dxi)[0]
        give_up.wait_recv()
        give_dn.wait_recv()
        for c in range(C):
            give_z[c].wait_recv()
        for k in range(3):
            for a in range(4):
                total = mine[k][a] * UNIT + rfm[4 * k + a] + rfp[4 * k + a] + rzm[a, k]
                f_out[k, a] = total
                speed = snd[a, 3 + k] + 0.5 * DT * total
                if last:
                    speed = jnp.where(present[a], speed, 0.0)
                else:
                    speed = snd[a, 3 + k]
                v_out[k, a] = speed
        if last:
            give_v.wait_recv()
            s_out[...] = stress + rfm[12] + rfp[12] + vzm[...]
    for copy in started:
        copy.wait_send()


def shards(mesh, positions, velocities, forces_prev, seeds, counts, offsets):
    ny, nz = mesh.shape["xy"], mesh.shape["gz"]
    f32, i32 = jnp.float32, jnp.int32
    vmem = pl.BlockSpec(memory_space=pltpu.VMEM)
    state0, state1 = (C, 7, 8, LANES), (C, 6, 8, LANES)
    scratch = [
        (state0, f32), (state1, f32), (state0, f32), (state1, f32), (state0, f32), (state1, f32),
        (state0, f32), (state1, f32),
        ((2, 12, 8, LANES), f32), ((2, 13, 8, LANES), f32),
        ((C, 3, 8, LANES), f32), ((C, 3, 8, LANES), f32), ((8, LANES), f32),
        ((12, 8, LANES), f32), ((13, 8, LANES), f32), ((12, 8, LANES), f32), ((13, 8, LANES), f32),
        ((C, 3, 8, LANES), f32), ((C, 3, 8, LANES), f32), ((8, LANES), f32),
        ((3, 6, C, 8, LANES), f32), ((3, 2, C, 8, LANES), i32),
        ((3, C, 6, 8, LANES), f32), ((3, C, 2, 8, LANES), i32),
        ((3, C, 6, 8, LANES), f32), ((3, C, 2, 8, LANES), i32),
        ((3, 3, 64, LANES), f32),
        ((3, 3, C, 8, LANES), f32), ((3, C, 3, 8, LANES), f32), ((3, 3, 8, LANES), f32),
        ((3, 6, 8, LANES), f32), ((3, 6, 8, LANES), f32), ((3, 6, 8, LANES), f32),
    ]
    force, speed, stress = pl.pallas_call(
        functools.partial(kernel, ny, nz),
        out_shape=(
            jax.ShapeDtypeStruct((3, C, 8, LANES), f32),
            jax.ShapeDtypeStruct((3, C, 8, LANES), f32),
            jax.ShapeDtypeStruct((8, LANES), f32),
        ),
        in_specs=[vmem] * 5 + [pl.BlockSpec(memory_space=pltpu.SMEM)],
        out_specs=(vmem, vmem, vmem),
        scratch_shapes=[pltpu.VMEM(shape, kind) for shape, kind in scratch]
        + [pltpu.SemaphoreType.DMA((2, 13)), pltpu.SemaphoreType.DMA((2, 13))],
        compiler_params=pltpu.CompilerParams(collective_id=0, has_side_effects=True),
    )(
        positions.reshape(3, C, 8, LANES),
        velocities.reshape(3, C, 8, LANES),
        forces_prev.reshape(3, C, 8, LANES),
        seeds.reshape(C, 8, LANES),
        counts.reshape(1, LANES),
        offsets,
    )
    return (
        force.reshape(3, 4 * 8, 1, 1, LANES),
        speed.reshape(3, 4 * 8, 1, 1, LANES),
        stress[:6].reshape(6, 1, 1, LANES),
    )


def solution(mesh):
    bead = P(None, None, "gz", "xy", None)
    return jax.shard_map(
        functools.partial(shards, mesh),
        mesh=mesh,
        in_specs=(bead, bead, bead, P(None, "gz", "xy", None), P("gz", "xy", None), P()),
        out_specs=(bead, bead, P(None, "gz", "xy", None)),
        check_vma=False,
    )
```

```python
import functools
import math

import jax
import jax.numpy as jnp
from jax import lax
from jax.experimental import pallas as pl
from jax.experimental.pallas import tpu as pltpu
from jax.sharding import PartitionSpec as P

DT = 0.04
PRIME = 65521
FAR = 1048576.0
NOISE = 3.0 * math.sqrt(12.0) / math.sqrt(DT)
UNIT = NOISE / 2.0**32
BIAS = 32768
OFFSET = 25.0 / UNIT - BIAS
DRAG = 4.5 / UNIT
PAIRS = [(0, 0), (1, 1), (2, 2), (0, 1), (0, 2), (1, 2)]
LANES = 128
C = 4


def phase(x):
    rest = jnp.floor(x.astype(jnp.float32) * (225.0 / PRIME) + 0.5).astype(jnp.int32)
    return x * jnp.int32(65551) + rest


def roll(x, shift):
    return pltpu.roll(x, shift, axis=x.ndim - 1)


def kernel(
    ny, nz, pos_in, vel_in, frc_in, seeds_in, counts_in, offsets_in, f_out, v_out, s_out,
    pos, vel, frc, seeds, counts, offsets, load,
    snd0, snd1, yn0, yn1, yf0, yf1, zp0, zp1, zm0, zm1, ry0, ry1, rz0, rz1, vz,
    rfn0, rfn1, rff0, rff1, rzm0, rzm1, vzm,
    ig, ii, jof, joi, jzf, jzi, jmf, jmi, gpart, facc, jacc_o, jacc_z, vi, vj_o, vj_z, send, recv,
):
    iy = lax.axis_index("xy")
    iz = lax.axis_index("gz")
    odd = lax.rem(iy, 2)
    side = 1.0 - 2.0 * odd.astype(jnp.float32)
    near_y = {"xy": iy + 1 - 2 * odd, "gz": iz}
    far_y = {"xy": lax.rem(iy + ny - 1 + 2 * odd, ny), "gz": iz}
    up_z = {"xy": iy, "gz": lax.rem(iz + 1, nz)}
    dn_z = {"xy": iy, "gz": lax.rem(iz + nz - 1, nz)}
    barrier = pltpu.get_barrier_semaphore()
    for where in (near_y, far_y, up_z, dn_z):
        pl.semaphore_signal(barrier, inc=1, device_id=where, device_id_type=pl.DeviceIdType.MESH)

    loads = [
        pltpu.make_async_copy(src, dst, load.at[n])
        for n, (src, dst) in enumerate(
            ((vel_in, vel), (frc_in, frc), (pos_in, pos), (counts_in, counts), (seeds_in, seeds), (offsets_in, offsets))
        )
    ]
    for copy in loads:
        copy.start()
    for copy in loads[:5]:
        copy.wait()

    started = []

    def remote(src, dst, step, slot, where):
        copy = pltpu.make_async_remote_copy(
            src_ref=src, dst_ref=dst, send_sem=send.at[step, slot], recv_sem=recv.at[step, slot],
            device_id=where, device_id_type=pl.DeviceIdType.MESH,
        )
        started.append(copy)
        return copy

    slot_no = (
        lax.broadcasted_iota(jnp.int32, (C, 8, LANES), 0) * 8 + lax.broadcasted_iota(jnp.int32, (C, 8, LANES), 1)
    )
    present = slot_no < counts[...]

    def tile(g, jf, ji, dxi, c, react, at, rows=range(4)):
        force = [{a: jnp.zeros((8, LANES), jnp.float32) for a in rows} for _ in range(3)]
        for j in range(8):
            near = [jnp.broadcast_to(jf[dxi, c, k, j : j + 1, :], (8, LANES)) for k in range(6)]
            seed_j = jnp.broadcast_to(ji[dxi, c, 0, j : j + 1, :], (8, LANES))
            base_j = jnp.broadcast_to(ji[dxi, c, 1, j : j + 1, :], (8, LANES))
            back = [None, None, None]
            for a in rows:
                d = [ig[g, k, a] - near[k] for k in range(3)]
                u = [ig[g, 3 + k, a] - near[3 + k] for k in range(3)]
                square = d[0] * d[0] + d[1] * d[1] + d[2] * d[2]
                inverse = lax.rsqrt(jnp.maximum(square, 0.0025))
                gap = jnp.maximum(inverse - 1.0, 0.0)
                drag = d[0] * u[0] + d[1] * u[1] + d[2] * u[2]
                angle = ii[g, 0, a] * seed_j + (ii[g, 1, a] + base_j)
                size = gap * ((angle.astype(jnp.float32) + OFFSET) - gap * drag)
                for k in range(3):
                    part = size * d[k]
                    force[k][a] = force[k][a] + part
                    if react:
                        back[k] = part if back[k] is None else back[k] + part
            if react:
                for k in range(3):
                    gpart[at, k, 8 * j : 8 * j + 8, :] = back[k]
        total = None
        if react:
            total = []
            for k in range(3):
                sums = [gpart[at, k, pl.ds(s, 8, stride=8), :] for s in range(8)]
                while len(sums) > 1:
                    sums = [sums[i] + sums[i + 1] for i in range(0, len(sums), 2)]
                total.append(sums[0])
        return force, total

    def pair_virial(g, jf, dxi, c, force, total):
        out = []
        for first, second in PAIRS:
            part = None
            for a in force[second]:
                term = ig[g, first, a] * force[second][a]
                part = term if part is None else part + term
            if total is None:
                part = part + part
            else:
                part = part - jf[dxi, c, first] * total[second]
            out.append(part)
        return out

    def add_force(g, forces):
        for k in range(3):
            for a in forces[0][k]:
                value = facc[g, k, a]
                for force in forces:
                    value = value + force[k][a]
                facc[g, k, a] = value

    def add_rows(ref, at, values):
        for k, value in enumerate(values):
            ref[(*at, k)] = ref[(*at, k)] + value

    def i_prep(g, block, seed, shift_y, shear, step, turn):
        for k in range(3):
            value = turn(block(k))
            if k == 1 and shift_y is not None:
                value = value + shift_y
            for a in range(4):
                ig[g, k, a] = value[a]
            speed = turn(block(3 + k))
            if k == 0 and shear is not None:
                speed = speed + shear
            speed = speed * DRAG
            for a in range(4):
                ig[g, 3 + k, a] = speed[a]
        first = turn(seed).astype(jnp.int32) + (7919 * step + 1)
        many = phase(2 * first + 1)
        alone = phase(first * (first + 1)) + jnp.int32(BIAS - 2**31)
        for a in range(4):
            ii[g, 0, a] = many[a]
            ii[g, 1, a] = alone[a]

    def j_prep(jf, c, value_of, shift_z):
        for k in range(6):
            value = value_of(c, k)
            if k == 2 and shift_z != 0.0:
                value = value + shift_z
            if k >= 3:
                value = value * DRAG
            for dxi in range(3):
                dx = dxi - 1
                moved = value if dx == 0 else roll(value, (-dx) % LANES)
                if k == 0 and dx != 0:
                    moved = moved + 2.0 * dx
                jf[dxi, c, k] = moved

    def j_seed(ji, c, seed):
        number = seed.astype(jnp.int32)
        base = phase(number * number)
        for dxi in range(3):
            dx = dxi - 1
            ji[dxi, c, 0] = number if dx == 0 else roll(number, (-dx) % LANES)
            ji[dxi, c, 1] = base if dx == 0 else roll(base, (-dx) % LANES)

    def back_to_place(values, dxi):
        dx = dxi - 1
        return [v if dx == 0 else roll(v, dx % LANES) for v in values]

    for step in range(2):
        last = step == 1
        snd, yn, yf, zp, zm = (snd1, yn1, yf1, zp1, zm1) if last else (snd0, yn0, yf0, zp0, zm0)
        ry, rz, rfn, rff, rzm = (ry1, rz1, rfn1, rff1, rzm1) if last else (ry0, rz0, rfn0, rff0, rzm0)
        for k in range(3):
            if not last:
                half = vel[k] + 0.5 * DT * frc[k]
                place = jnp.where(present, pos[k] + DT * half, FAR)
            else:
                half = v_out[k] + DT * f_out[k]
                old = jnp.stack([snd0[c, k] for c in range(C)])
                place = jnp.where(present, old + DT * half, FAR)
            for c in range(C):
                snd[c, k] = place[c]
                snd[c, 3 + k] = half[c]
        if not last:
            number = seeds[...].astype(jnp.float32)
            for c in range(C):
                snd[c, 6] = number[c]

        def own(k):
            return jnp.stack([snd[c, k] for c in range(C)])

        seed_own = jnp.stack([snd0[c, 6] for c in range(C)])
        i_prep(0, own, seed_own, None, None, step, lambda v: v)
        if not last:
            pl.semaphore_wait(barrier, 4)
        send_z = [remote(snd.at[c], zp.at[c], step, c, dn_z) for c in range(C)]
        send_near = remote(snd, yn, step, 4, near_y)
        send_far = remote(snd, yf, step, 5, far_y)
        send_near.start()
        for c in range(C):
            send_z[c].start()
        send_far.start()
        send_lower = remote(snd.at[pl.ds(2, 2)], zm, step, 13, up_z)
        send_lower.start()

        for c in range(C):
            j_prep(jof, c, lambda c, k: snd[c, k], 0.0)
            if not last:
                j_seed(joi, c, snd0[c, 6])
        zero = jnp.zeros((8, LANES), jnp.float32)
        for g in range(3):
            for k in range(3):
                for a in range(4):
                    facc[g, k, a] = zero
            if last:
                for k in range(6):
                    vi[g, k] = zero
                    vj_o[g, k] = zero
                    vj_z[g, k] = zero

        def own_body(c, carry):
            force, _ = tile(0, jof, joi, 1, c, False, 0)
            force_x, total_x = tile(0, jof, joi, 2, c, True, 0)
            add_force(0, [force, force_x])
            for k in range(3):
                jacc_o[0, c, k] = jnp.zeros((8, LANES), jnp.float32)
                jacc_o[1, c, k] = jnp.zeros((8, LANES), jnp.float32)
                jacc_o[2, c, k] = total_x[k]
            if last:
                add_rows(vi, (0,), pair_virial(0, jof, 1, c, force, None))
                part = pair_virial(0, jof, 2, c, force_x, total_x)
                add_rows(vi, (0,), part)
                add_rows(vj_o, (2,), part)
            return carry

        lax.fori_loop(0, C, own_body, 0)

        def multi(g, jf, ji, c, jacc, vj, rows=range(4)):
            forces = []
            for dxi in range(3):
                force, total = tile(g, jf, ji, dxi, c, last or jacc is not None, dxi, rows)
                forces.append(force)
                if jacc is not None:
                    add_rows(jacc, (dxi, c), total)
                if last:
                    part = pair_virial(g, jf, dxi, c, force, total)
                    add_rows(vi, (g,), part)
                    if vj is not None:
                        add_rows(vj, (dxi,), part)
            add_force(g, forces)

        def pair_own(g):
            def body(c, carry):
                multi(g, jof, joi, c, jacc_o, vj_o)
                return carry

            lax.fori_loop(0, C, body, 0)

        def pair_z(jf, ji, chunks, rows):
            def body(c, carry):
                multi(0, jf, ji, c, None, None, rows)
                return carry

            lax.fori_loop(0, chunks, body, 0)

        scale = UNIT * 0.5 / 8.0

        def virial_rows(ref, at):
            rows = [jnp.sum(ref[at, k], axis=0, keepdims=True) for k in range(6)]
            return jnp.concatenate(rows + [jnp.zeros((2, LANES), jnp.float32)], axis=0) * scale

        send_near.wait_recv()
        i_prep(
            1, lambda k: jnp.stack([yn[c, k] for c in range(C)]), jnp.stack([yn0[c, 6] for c in range(C)]),
            2.0 * side, None, step, lambda v: v,
        )

        @pl.when(odd == 0)
        def _():
            pair_own(1)

        def near_body(c, carry):
            pltpu.make_async_remote_copy(
                src_ref=snd.at[c], dst_ref=zp.at[c], send_sem=send.at[step, c], recv_sem=recv.at[step, c],
                device_id=dn_z, device_id_type=pl.DeviceIdType.MESH,
            ).wait_recv()
            j_prep(jzf, c, lambda c, k: zp[c, k], 2.0)
            if not last:
                j_seed(jzi, c, zp0[c, 6])
            for dxi in range(3):
                for k in range(3):
                    jacc_z[dxi, c, k] = zero
            multi(1, jzf, jzi, c, jacc_z, vj_z)
            multi(0, jzf, jzi, c, jacc_z, vj_z, (0, 1))
            return carry

        lax.fori_loop(0, C, near_body, 0)

        for k in range(3):
            for a in range(4):
                ry[0, 4 * k + a] = facc[1, k, a] * UNIT
        if last:
            ry[0, 12] = virial_rows(vi, 1)
        give_near = remote(ry.at[0], rfn, step, 10, near_y)
        give_near.start()

        if not last:
            loads[5].wait()
        offset = offsets[step]
        top = iy == ny - 1
        bottom = iy == 0
        turn = jnp.where(top, offset, jnp.where(bottom, lax.rem(LANES - offset, LANES), 0))
        undo = lax.rem(LANES - turn, LANES)
        shear = jnp.where(top, 1.0, jnp.where(bottom, -1.0, 0.0))
        send_far.wait_recv()
        i_prep(
            2, lambda k: jnp.stack([yf[c, k] for c in range(C)]), jnp.stack([yf0[c, 6] for c in range(C)]),
            -2.0 * side, shear, step, lambda v: jnp.stack([roll(v[a], turn) for a in range(C)]),
        )

        def give_chunk(c):
            return pltpu.make_async_remote_copy(
                src_ref=rz.at[c], dst_ref=rzm.at[c], send_sem=send.at[step, 6 + c], recv_sem=recv.at[step, 6 + c],
                device_id=up_z, device_id_type=pl.DeviceIdType.MESH,
            )

        def far_body(c, carry):
            multi(2, jzf, jzi, c, jacc_z, vj_z)
            for k in range(3):
                value = zero
                for dxi in range(3):
                    value = value + back_to_place([jacc_z[dxi, c, k]], dxi)[0]
                rz[c, k] = value * (-UNIT)
            give_chunk(c).start()
            return carry

        lax.fori_loop(0, C, far_body, 0)
        give_z = [give_chunk(c) for c in range(C)]
        started.extend(give_z)
        if last:
            value = zero
            for dxi in range(3):
                value = value + back_to_place([virial_rows(vj_z, dxi)], dxi)[0]
            vz[...] = value
            give_v = remote(vz, vzm, step, 12, up_z)
            give_v.start()

        @pl.when(odd == 1)
        def _():
            pair_own(2)

        for k in range(3):
            for a in range(4):
                ry[1, 4 * k + a] = roll(facc[2, k, a] * UNIT, undo)
        if last:
            ry[1, 12] = roll(virial_rows(vi, 2), undo)
        give_far = remote(ry.at[1], rff, step, 11, far_y)
        give_far.start()

        pair_z(jzf, jzi, C, (2, 3))
        send_lower.wait_recv()
        for c in range(2):
            j_prep(jmf, c, lambda c, k: zm[c, k], -2.0)
            if not last:
                j_seed(jmi, c, zm0[c, 6])
        pair_z(jmf, jmi, 2, range(4))

        mine = [[facc[0, k, a] for a in range(4)] for k in range(3)]
        for dxi in range(3):
            for k in range(3):
                moved = back_to_place([jacc_o[dxi, a, k] for a in range(4)], dxi)
                mine[k] = [mine[k][a] - moved[a] for a in range(4)]
        if last:
            stress = virial_rows(vi, 0)
            for dxi in range(3):
                stress = stress + back_to_place([virial_rows(vj_o, dxi)], dxi)[0]
        give_near.wait_recv()
        for c in range(C):
            give_z[c].wait_recv()
        give_far.wait_recv()
        for k in range(3):
            for a in range(4):
                total = mine[k][a] * UNIT + rfn[4 * k + a] + rff[4 * k + a] + rzm[a, k]
                f_out[k, a] = total
                speed = snd[a, 3 + k] + 0.5 * DT * total
                if last:
                    speed = jnp.where(present[a], speed, 0.0)
                else:
                    speed = snd[a, 3 + k]
                v_out[k, a] = speed
        if last:
            give_v.wait_recv()
            stress = stress + rfn[12] + rff[12] + vzm[...]
            for k in range(6):
                s_out[k] = stress[k : k + 1, :]
    for copy in started:
        copy.wait_send()


def shards(mesh, positions, velocities, forces_prev, seeds, counts, offsets):
    ny, nz = mesh.shape["xy"], mesh.shape["gz"]
    f32, i32 = jnp.float32, jnp.int32
    vmem = pl.BlockSpec(memory_space=pltpu.VMEM)
    state0, state1 = (C, 7, 8, LANES), (C, 6, 8, LANES)
    bead = (3, C, 8, LANES)
    scratch = [(state0, f32), (state1, f32)] * 4 + [((2, 7, 8, LANES), f32), ((2, 6, 8, LANES), f32)] + [
        ((2, 12, 8, LANES), f32), ((2, 13, 8, LANES), f32),
        ((C, 3, 8, LANES), f32), ((C, 3, 8, LANES), f32), ((8, LANES), f32),
        ((12, 8, LANES), f32), ((13, 8, LANES), f32), ((12, 8, LANES), f32), ((13, 8, LANES), f32),
        ((C, 3, 8, LANES), f32), ((C, 3, 8, LANES), f32), ((8, LANES), f32),
        ((3, 6, C, 8, LANES), f32), ((3, 2, C, 8, LANES), i32),
        ((3, C, 6, 8, LANES), f32), ((3, C, 2, 8, LANES), i32),
        ((3, C, 6, 8, LANES), f32), ((3, C, 2, 8, LANES), i32),
        ((3, C, 6, 8, LANES), f32), ((3, C, 2, 8, LANES), i32),
        ((3, 3, 64, LANES), f32),
        ((3, 3, C, 8, LANES), f32), ((3, C, 3, 8, LANES), f32), ((3, C, 3, 8, LANES), f32),
        ((3, 6, 8, LANES), f32), ((3, 6, 8, LANES), f32), ((3, 6, 8, LANES), f32),
    ]
    inputs = [(bead, f32), (bead, f32), (bead, f32), ((C, 8, LANES), i32), ((1, LANES), i32)]
    force, speed, stress = pl.pallas_call(
        functools.partial(kernel, ny, nz),
        out_shape=(pltpu.VMEM(bead, f32), pltpu.VMEM(bead, f32), pltpu.VMEM((6, 1, LANES), f32)),
        in_specs=[pl.BlockSpec(memory_space=pl.ANY)] * 6,
        out_specs=(vmem, vmem, vmem),
        scratch_shapes=[pltpu.VMEM(shape, kind) for shape, kind in inputs]
        + [pltpu.SMEM((2,), i32), pltpu.SemaphoreType.DMA((6,))]
        + [pltpu.VMEM(shape, kind) for shape, kind in scratch]
        + [pltpu.SemaphoreType.DMA((2, 14)), pltpu.SemaphoreType.DMA((2, 14))],
        compiler_params=pltpu.CompilerParams(collective_id=0, has_side_effects=True),
    )(
        positions.reshape(bead),
        velocities.reshape(bead),
        forces_prev.reshape(bead),
        seeds.reshape(C, 8, LANES),
        counts.reshape(1, LANES),
        offsets,
    )
    return (
        force.reshape(3, 4 * 8, 1, 1, LANES),
        speed.reshape(3, 4 * 8, 1, 1, LANES),
        stress.reshape(6, 1, 1, LANES),
    )


def solution(mesh):
    bead = P(None, None, "gz", "xy", None)
    return jax.shard_map(
        functools.partial(shards, mesh),
        mesh=mesh,
        in_specs=(bead, bead, bead, P(None, "gz", "xy", None), P("gz", "xy", None), P()),
        out_specs=(bead, bead, P(None, "gz", "xy", None)),
        check_vma=False,
    )
```

```python
import functools
import math

import jax
import jax.numpy as jnp
from jax import lax
from jax.experimental import pallas as pl
from jax.experimental.pallas import tpu as pltpu
from jax.sharding import PartitionSpec as P

DT = 0.04
PRIME = 65521
FAR = 1048576.0
NOISE = 3.0 * math.sqrt(12.0) / math.sqrt(DT)
UNIT = NOISE / 2.0**32
BIAS = 32768
OFFSET = 25.0 / UNIT - BIAS
DRAG = 4.5 / UNIT
PAIRS = [(0, 0), (1, 1), (2, 2), (0, 1), (0, 2), (1, 2)]
LANES = 128
C = 4


def phase(x):
    rest = jnp.floor(x.astype(jnp.float32) * (225.0 / PRIME) + 0.5).astype(jnp.int32)
    return x * jnp.int32(65551) + rest


def roll(x, shift):
    return pltpu.roll(x, shift, axis=x.ndim - 1)


def kernel(
    ny, nz, pos_in, vel_in, frc_in, seeds_in, counts_in, offsets_in, f_out, v_out, s_out,
    pos, vel, frc, seeds, counts, offsets, load,
    snd0, snd1, yn0, yn1, yf0, yf1, zp0, zp1, zm0, zm1, ry0, ry1, rz0, rz1, vz,
    rfn0, rfn1, rff0, rff1, rzm0, rzm1, vzm,
    ig, ii, jof, joi, jzf, jzi, jmf, jmi, gpart, facc, jacc_o, jacc_z, vi, vj_o, vj_z, send, recv,
):
    iy = lax.axis_index("xy")
    iz = lax.axis_index("gz")
    odd = lax.rem(iy, 2)
    side = 1.0 - 2.0 * odd.astype(jnp.float32)
    near_y = {"xy": iy + 1 - 2 * odd, "gz": iz}
    far_y = {"xy": lax.rem(iy + ny - 1 + 2 * odd, ny), "gz": iz}
    up_z = {"xy": iy, "gz": lax.rem(iz + 1, nz)}
    dn_z = {"xy": iy, "gz": lax.rem(iz + nz - 1, nz)}
    barrier = pltpu.get_barrier_semaphore()
    for where in (near_y, far_y, up_z, dn_z):
        pl.semaphore_signal(barrier, inc=1, device_id=where, device_id_type=pl.DeviceIdType.MESH)

    loads = [
        pltpu.make_async_copy(src, dst, load.at[n])
        for n, (src, dst) in enumerate(
            ((vel_in, vel), (frc_in, frc), (pos_in, pos), (counts_in, counts), (seeds_in, seeds), (offsets_in, offsets))
        )
    ]
    for copy in loads:
        copy.start()
    for copy in loads[:5]:
        copy.wait()

    started = []
    lowers = []

    def remote(src, dst, step, slot, where):
        copy = pltpu.make_async_remote_copy(
            src_ref=src, dst_ref=dst, send_sem=send.at[step, slot], recv_sem=recv.at[step, slot],
            device_id=where, device_id_type=pl.DeviceIdType.MESH,
        )
        started.append(copy)
        return copy

    slot_no = (
        lax.broadcasted_iota(jnp.int32, (C, 8, LANES), 0) * 8 + lax.broadcasted_iota(jnp.int32, (C, 8, LANES), 1)
    )
    present = slot_no < counts[...]

    def tile(g, jf, ji, dxi, c, react, at, rows=range(4)):
        force = [{a: jnp.zeros((8, LANES), jnp.float32) for a in rows} for _ in range(3)]
        for j in range(8):
            near = [jnp.broadcast_to(jf[dxi, c, k, j : j + 1, :], (8, LANES)) for k in range(6)]
            seed_j = jnp.broadcast_to(ji[dxi, c, 0, j : j + 1, :], (8, LANES))
            base_j = jnp.broadcast_to(ji[dxi, c, 1, j : j + 1, :], (8, LANES))
            back = [None, None, None]
            for a in rows:
                d = [ig[g, k, a] - near[k] for k in range(3)]
                u = [ig[g, 3 + k, a] - near[3 + k] for k in range(3)]
                square = d[0] * d[0] + d[1] * d[1] + d[2] * d[2]
                inverse = lax.rsqrt(jnp.maximum(square, 0.0025))
                gap = jnp.maximum(inverse - 1.0, 0.0)
                drag = d[0] * u[0] + d[1] * u[1] + d[2] * u[2]
                angle = ii[g, 0, a] * seed_j + (ii[g, 1, a] + base_j)
                size = gap * ((angle.astype(jnp.float32) + OFFSET) - gap * drag)
                for k in range(3):
                    part = size * d[k]
                    force[k][a] = force[k][a] + part
                    if react:
                        back[k] = part if back[k] is None else back[k] + part
            if react:
                for k in range(3):
                    gpart[at, k, 8 * j : 8 * j + 8, :] = back[k]
        total = None
        if react:
            total = []
            for k in range(3):
                sums = [gpart[at, k, pl.ds(s, 8, stride=8), :] for s in range(8)]
                while len(sums) > 1:
                    sums = [sums[i] + sums[i + 1] for i in range(0, len(sums), 2)]
                total.append(sums[0])
        return force, total

    def pair_virial(g, jf, dxi, c, force, total):
        out = []
        for first, second in PAIRS:
            part = None
            for a in force[second]:
                term = ig[g, first, a] * force[second][a]
                part = term if part is None else part + term
            if total is None:
                part = part + part
            else:
                part = part - jf[dxi, c, first] * total[second]
            out.append(part)
        return out

    def add_force(g, forces):
        for k in range(3):
            for a in forces[0][k]:
                value = facc[g, k, a]
                for force in forces:
                    value = value + force[k][a]
                facc[g, k, a] = value

    def add_rows(ref, at, values):
        for k, value in enumerate(values):
            ref[(*at, k)] = ref[(*at, k)] + value

    def i_prep(g, block, seed, shift_y, shear, step, turn):
        for k in range(3):
            value = turn(block(k))
            if k == 1 and shift_y is not None:
                value = value + shift_y
            for a in range(4):
                ig[g, k, a] = value[a]
            speed = turn(block(3 + k))
            if k == 0 and shear is not None:
                speed = speed + shear
            speed = speed * DRAG
            for a in range(4):
                ig[g, 3 + k, a] = speed[a]
        first = turn(seed).astype(jnp.int32) + (7919 * step + 1)
        many = phase(2 * first + 1)
        alone = phase(first * (first + 1)) + jnp.int32(BIAS - 2**31)
        for a in range(4):
            ii[g, 0, a] = many[a]
            ii[g, 1, a] = alone[a]

    def j_prep(jf, c, value_of, shift_z):
        for k in range(6):
            value = value_of(c, k)
            if k == 2 and shift_z != 0.0:
                value = value + shift_z
            if k >= 3:
                value = value * DRAG
            for dxi in range(3):
                dx = dxi - 1
                moved = value if dx == 0 else roll(value, (-dx) % LANES)
                if k == 0 and dx != 0:
                    moved = moved + 2.0 * dx
                jf[dxi, c, k] = moved

    def j_seed(ji, c, seed):
        number = seed.astype(jnp.int32)
        base = phase(number * number)
        for dxi in range(3):
            dx = dxi - 1
            ji[dxi, c, 0] = number if dx == 0 else roll(number, (-dx) % LANES)
            ji[dxi, c, 1] = base if dx == 0 else roll(base, (-dx) % LANES)

    def back_to_place(values, dxi):
        dx = dxi - 1
        return [v if dx == 0 else roll(v, dx % LANES) for v in values]

    for step in range(2):
        last = step == 1
        snd, yn, yf, zp, zm = (snd1, yn1, yf1, zp1, zm1) if last else (snd0, yn0, yf0, zp0, zm0)
        ry, rz, rfn, rff, rzm = (ry1, rz1, rfn1, rff1, rzm1) if last else (ry0, rz0, rfn0, rff0, rzm0)
        for k in range(3):
            if not last:
                half = vel[k] + 0.5 * DT * frc[k]
                place = jnp.where(present, pos[k] + DT * half, FAR)
            else:
                half = v_out[k] + DT * f_out[k]
                old = jnp.stack([snd0[c, k] for c in range(C)])
                place = jnp.where(present, old + DT * half, FAR)
            for c in range(C):
                snd[c, k] = place[c]
                snd[c, 3 + k] = half[c]
        if not last:
            number = seeds[...].astype(jnp.float32)
            for c in range(C):
                snd[c, 6] = number[c]

        def own(k):
            return jnp.stack([snd[c, k] for c in range(C)])

        seed_own = jnp.stack([snd0[c, 6] for c in range(C)])
        i_prep(0, own, seed_own, None, None, step, lambda v: v)
        if not last:
            pl.semaphore_wait(barrier, 4)
        send_z = [remote(snd.at[c], zp.at[c], step, c, dn_z) for c in range(C)]
        send_near = remote(snd, yn, step, 4, near_y)
        send_far = remote(snd, yf, step, 5, far_y)
        send_near.start()
        for c in range(C):
            send_z[c].start()
        send_far.start()
        send_lower = pltpu.make_async_remote_copy(
            src_ref=snd, dst_ref=zm, send_sem=send.at[step, 13], recv_sem=recv.at[step, 13],
            device_id=up_z, device_id_type=pl.DeviceIdType.MESH,
        )
        lowers.append(send_lower)

        @pl.when(odd == 0)
        def _():
            send_lower.start()


        for c in range(C):
            j_prep(jof, c, lambda c, k: snd[c, k], 0.0)
            if not last:
                j_seed(joi, c, snd0[c, 6])
        zero = jnp.zeros((8, LANES), jnp.float32)
        for g in range(3):
            for k in range(3):
                for a in range(4):
                    facc[g, k, a] = zero
            if last:
                for k in range(6):
                    vi[g, k] = zero
                    vj_o[g, k] = zero
                    vj_z[g, k] = zero

        def own_body(c, carry):
            force, _ = tile(0, jof, joi, 1, c, False, 0)
            force_x, total_x = tile(0, jof, joi, 2, c, True, 0)
            add_force(0, [force, force_x])
            for k in range(3):
                jacc_o[0, c, k] = jnp.zeros((8, LANES), jnp.float32)
                jacc_o[1, c, k] = jnp.zeros((8, LANES), jnp.float32)
                jacc_o[2, c, k] = total_x[k]
            if last:
                add_rows(vi, (0,), pair_virial(0, jof, 1, c, force, None))
                part = pair_virial(0, jof, 2, c, force_x, total_x)
                add_rows(vi, (0,), part)
                add_rows(vj_o, (2,), part)
            return carry

        lax.fori_loop(0, C, own_body, 0)

        def multi(g, jf, ji, c, jacc, vj, rows=range(4)):
            forces = []
            for dxi in range(3):
                force, total = tile(g, jf, ji, dxi, c, last or jacc is not None, dxi, rows)
                forces.append(force)
                if jacc is not None:
                    add_rows(jacc, (dxi, c), total)
                if last:
                    part = pair_virial(g, jf, dxi, c, force, total)
                    add_rows(vi, (g,), part)
                    if vj is not None:
                        add_rows(vj, (dxi,), part)
            add_force(g, forces)

        def pair_own(g):
            def body(c, carry):
                multi(g, jof, joi, c, jacc_o, vj_o)
                return carry

            lax.fori_loop(0, C, body, 0)

        def pair_z(jf, ji):
            def body(c, carry):
                multi(0, jf, ji, c, None, None)
                return carry

            lax.fori_loop(0, C, body, 0)

        scale = UNIT * 0.5 / 8.0

        def virial_rows(ref, at):
            rows = [jnp.sum(ref[at, k], axis=0, keepdims=True) for k in range(6)]
            return jnp.concatenate(rows + [jnp.zeros((2, LANES), jnp.float32)], axis=0) * scale

        send_near.wait_recv()
        i_prep(
            1, lambda k: jnp.stack([yn[c, k] for c in range(C)]), jnp.stack([yn0[c, 6] for c in range(C)]),
            2.0 * side, None, step, lambda v: v,
        )

        @pl.when(odd == 0)
        def _():
            pair_own(1)

        def near_body(both, c, carry):
            pltpu.make_async_remote_copy(
                src_ref=snd.at[c], dst_ref=zp.at[c], send_sem=send.at[step, c], recv_sem=recv.at[step, c],
                device_id=dn_z, device_id_type=pl.DeviceIdType.MESH,
            ).wait_recv()
            j_prep(jzf, c, lambda c, k: zp[c, k], 2.0)
            if not last:
                j_seed(jzi, c, zp0[c, 6])
            for dxi in range(3):
                for k in range(3):
                    jacc_z[dxi, c, k] = zero
            multi(1, jzf, jzi, c, jacc_z, vj_z)
            if both:
                multi(0, jzf, jzi, c, jacc_z, vj_z)
            return carry

        @pl.when(odd == 0)
        def _():
            lax.fori_loop(0, C, functools.partial(near_body, False), 0)

        @pl.when(odd == 1)
        def _():
            lax.fori_loop(0, C, functools.partial(near_body, True), 0)

        for k in range(3):
            for a in range(4):
                ry[0, 4 * k + a] = facc[1, k, a] * UNIT
        if last:
            ry[0, 12] = virial_rows(vi, 1)
        give_near = remote(ry.at[0], rfn, step, 10, near_y)
        give_near.start()

        if not last:
            loads[5].wait()
        offset = offsets[step]
        top = iy == ny - 1
        bottom = iy == 0
        turn = jnp.where(top, offset, jnp.where(bottom, lax.rem(LANES - offset, LANES), 0))
        undo = lax.rem(LANES - turn, LANES)
        shear = jnp.where(top, 1.0, jnp.where(bottom, -1.0, 0.0))
        send_far.wait_recv()
        i_prep(
            2, lambda k: jnp.stack([yf[c, k] for c in range(C)]), jnp.stack([yf0[c, 6] for c in range(C)]),
            -2.0 * side, shear, step, lambda v: jnp.stack([roll(v[a], turn) for a in range(C)]),
        )

        def give_chunk(c):
            return pltpu.make_async_remote_copy(
                src_ref=rz.at[c], dst_ref=rzm.at[c], send_sem=send.at[step, 6 + c], recv_sem=recv.at[step, 6 + c],
                device_id=up_z, device_id_type=pl.DeviceIdType.MESH,
            )

        def far_body(c, carry):
            multi(2, jzf, jzi, c, jacc_z, vj_z)
            for k in range(3):
                value = zero
                for dxi in range(3):
                    value = value + back_to_place([jacc_z[dxi, c, k]], dxi)[0]
                rz[c, k] = value * (-UNIT)
            give_chunk(c).start()
            return carry

        lax.fori_loop(0, C, far_body, 0)
        give_z = [give_chunk(c) for c in range(C)]
        started.extend(give_z)
        if last:
            value = zero
            for dxi in range(3):
                value = value + back_to_place([virial_rows(vj_z, dxi)], dxi)[0]
            vz[...] = value
            give_v = remote(vz, vzm, step, 12, up_z)
            give_v.start()

        @pl.when(odd == 1)
        def _():
            pair_own(2)

        for k in range(3):
            for a in range(4):
                ry[1, 4 * k + a] = roll(facc[2, k, a] * UNIT, undo)
        if last:
            ry[1, 12] = roll(virial_rows(vi, 2), undo)
        give_far = remote(ry.at[1], rff, step, 11, far_y)
        give_far.start()

        @pl.when(odd == 0)
        def _():
            pair_z(jzf, jzi)
            send_lower.wait_recv()
            for c in range(C):
                j_prep(jmf, c, lambda c, k: zm[c, k], -2.0)
                if not last:
                    j_seed(jmi, c, zm0[c, 6])
            pair_z(jmf, jmi)

        mine = [[facc[0, k, a] for a in range(4)] for k in range(3)]
        for dxi in range(3):
            for k in range(3):
                moved = back_to_place([jacc_o[dxi, a, k] for a in range(4)], dxi)
                mine[k] = [mine[k][a] - moved[a] for a in range(4)]
        if last:
            stress = virial_rows(vi, 0)
            for dxi in range(3):
                stress = stress + back_to_place([virial_rows(vj_o, dxi)], dxi)[0]
        give_near.wait_recv()
        for c in range(C):
            give_z[c].wait_recv()
        give_far.wait_recv()
        for k in range(3):
            for a in range(4):
                total = mine[k][a] * UNIT + rfn[4 * k + a] + rff[4 * k + a] + rzm[a, k]
                f_out[k, a] = total
                speed = snd[a, 3 + k] + 0.5 * DT * total
                if last:
                    speed = jnp.where(present[a], speed, 0.0)
                else:
                    speed = snd[a, 3 + k]
                v_out[k, a] = speed
        if last:
            give_v.wait_recv()
            stress = stress + rfn[12] + rff[12] + vzm[...]
            for k in range(6):
                s_out[k] = stress[k : k + 1, :]
    for copy in started:
        copy.wait_send()

    @pl.when(odd == 0)
    def _():
        for copy in lowers:
            copy.wait_send()


def shards(mesh, positions, velocities, forces_prev, seeds, counts, offsets):
    ny, nz = mesh.shape["xy"], mesh.shape["gz"]
    f32, i32 = jnp.float32, jnp.int32
    vmem = pl.BlockSpec(memory_space=pltpu.VMEM)
    state0, state1 = (C, 7, 8, LANES), (C, 6, 8, LANES)
    bead = (3, C, 8, LANES)
    scratch = [(state0, f32), (state1, f32)] * 5 + [
        ((2, 12, 8, LANES), f32), ((2, 13, 8, LANES), f32),
        ((C, 3, 8, LANES), f32), ((C, 3, 8, LANES), f32), ((8, LANES), f32),
        ((12, 8, LANES), f32), ((13, 8, LANES), f32), ((12, 8, LANES), f32), ((13, 8, LANES), f32),
        ((C, 3, 8, LANES), f32), ((C, 3, 8, LANES), f32), ((8, LANES), f32),
        ((3, 6, C, 8, LANES), f32), ((3, 2, C, 8, LANES), i32),
        ((3, C, 6, 8, LANES), f32), ((3, C, 2, 8, LANES), i32),
        ((3, C, 6, 8, LANES), f32), ((3, C, 2, 8, LANES), i32),
        ((3, C, 6, 8, LANES), f32), ((3, C, 2, 8, LANES), i32),
        ((3, 3, 64, LANES), f32),
        ((3, 3, C, 8, LANES), f32), ((3, C, 3, 8, LANES), f32), ((3, C, 3, 8, LANES), f32),
        ((3, 6, 8, LANES), f32), ((3, 6, 8, LANES), f32), ((3, 6, 8, LANES), f32),
    ]
    inputs = [(bead, f32), (bead, f32), (bead, f32), ((C, 8, LANES), i32), ((1, LANES), i32)]
    force, speed, stress = pl.pallas_call(
        functools.partial(kernel, ny, nz),
        out_shape=(pltpu.VMEM(bead, f32), pltpu.VMEM(bead, f32), pltpu.VMEM((6, 1, LANES), f32)),
        in_specs=[pl.BlockSpec(memory_space=pl.ANY)] * 6,
        out_specs=(vmem, vmem, vmem),
        scratch_shapes=[pltpu.VMEM(shape, kind) for shape, kind in inputs]
        + [pltpu.SMEM((2,), i32), pltpu.SemaphoreType.DMA((6,))]
        + [pltpu.VMEM(shape, kind) for shape, kind in scratch]
        + [pltpu.SemaphoreType.DMA((2, 14)), pltpu.SemaphoreType.DMA((2, 14))],
        compiler_params=pltpu.CompilerParams(collective_id=0, has_side_effects=True),
    )(
        positions.reshape(bead),
        velocities.reshape(bead),
        forces_prev.reshape(bead),
        seeds.reshape(C, 8, LANES),
        counts.reshape(1, LANES),
        offsets,
    )
    return (
        force.reshape(3, 4 * 8, 1, 1, LANES),
        speed.reshape(3, 4 * 8, 1, 1, LANES),
        stress.reshape(6, 1, 1, LANES),
    )


def solution(mesh):
    bead = P(None, None, "gz", "xy", None)
    return jax.shard_map(
        functools.partial(shards, mesh),
        mesh=mesh,
        in_specs=(bead, bead, bead, P(None, "gz", "xy", None), P("gz", "xy", None), P()),
        out_specs=(bead, bead, P(None, "gz", "xy", None)),
        check_vma=False,
    )
```
